256 devices in a mesh: seq: 64 (over z, y, core), head: 4 (over x).
Axes of the slice: x: 4, y: 4, z: 8, core: 2. Of those that a mesh axis runs over, the one named last changes fastest.
Arguments:
- query: bfloat16 [128, 32, 128], P(None, 'head'), may hold values from -8 to 8
- key_cache: bfloat16 [131072, 16, 128], P('seq', 'head'), may hold values from -6 to 6
- value_cache: bfloat16 [131072, 16, 128], P('seq', 'head'), may hold values from -6 to 6
- lengths: int32 [64], P('seq'), may hold values from 1 to 2048, 98304 in all
- out_weight: bfloat16 [4608, 4096], P('seq', 'head'), may hold values from -10 to 10
- norm_gain: float32 [4608], P('seq'), may hold values from 0.1 to 1.9
Outputs:
- normed: bfloat16 [128, 4608], P(None, 'seq')
The draws below stay inside these ranges and needn't reach their ends.
Inputs may be any that keep to these rules, and one draw needn't show every extreme that they name: `lengths`: every block has at least one valid position, and some block is valid throughout.
All inputs are finite; a program needn't handle non-finite values.
Results may differ from the reference program's by a relative error of at most 0.0083.
Values may be sent and summed in bfloat16 or wider, within the bound.
A program may use at most 128 MiB of HBM per device.

```python
import math
import jax
import jax.numpy as jnp
import numpy as np
from jax import lax

D = 4608
HEADS = 32
KVH = 16
HD = 128
QTOK = 128
CACHE_DEV = 2048
CACHE = 131072
QPRE = 144
N_SEQ = 64


def draw_query(key, part):
    folded = jax.random.fold_in(key, 11)
    base = jnp.clip(1.5 * jax.random.normal(folded, (QTOK, HEADS, HD), jnp.float32), -8.0, 8.0)
    return base.astype(jnp.bfloat16)


def draw_key_cache(key, part):
    folded = jax.random.fold_in(key, 23)
    base = jnp.clip(jax.random.normal(folded, (CACHE, KVH, HD), jnp.float32), -6.0, 6.0)
    return base.astype(jnp.bfloat16)


def draw_out_weight(key, part):
    folded = jax.random.fold_in(key, 37)
    key_entries, key_scales = jax.random.split(folded)
    position = jnp.arange(D, dtype=jnp.float32) / D
    row_scales = jnp.exp(jax.random.uniform(key_scales, (D,), jnp.float32, 0.0, math.log(10.0)))
    entries = jnp.clip(jax.random.normal(key_entries, (D, HEADS * HD), jnp.float32), -4.0, 4.0)
    trend = 1.0 + 2.0 * position
    weight_rows = entries * (row_scales * trend)[:, None] / math.sqrt(HEADS * HD)
    return weight_rows.astype(jnp.bfloat16)


def level_of(rng, extent, cuts, low, largest):
    loudness = 1.0
    for axis_at, parts in cuts:
        draws = jax.random.uniform(jax.random.fold_in(jax.random.fold_in(rng, 6), axis_at), (parts,), jnp.float32, low / len(cuts), largest / len(cuts))
        loudness = loudness * jnp.repeat(jnp.exp(draws), extent[axis_at] // parts).reshape((-1,) + (1,) * (len(extent) - 1 - axis_at))
    return loudness


def profile(number_of, total, bound, slope):
    portions = [(1 << 20) // math.isqrt(standing ** slope) + 1 for standing in range(2, number_of + 1)]
    spare, holding = total - bound - (number_of - 1), [1] * (number_of - 1)
    while spare > 0:
        candidates = [i for i in range(number_of - 1) if holding[i] < bound]
        pool, left = sum([portions[i] for i in candidates]), spare
        for i in candidates:
            extra = min(bound - holding[i], max(1, left * portions[i] // pool), spare)
            holding[i] = holding[i] + extra
            spare = spare - extra
    return np.array([bound] + holding)


def ragged_sizes(stream_key, amount, total, most, skew):
    if amount == 2:
        one = jax.random.randint(stream_key, (), max(1, total - most), min(most, total - 1) + 1)
        return jnp.stack([one, total - one])
    sizes = jnp.asarray(profile(amount, total, most, skew), jnp.int32)
    couples = (amount - 1) // 2
    source_of, taker = sizes[1:1 + 2 * couples:2], sizes[2:2 + 2 * couples:2]
    margin = jnp.minimum(source_of - 1, most - taker)
    moved = jax.random.randint(jax.random.fold_in(stream_key, 1), (couples,), 0, 1 << 20) % (margin + 1)
    sizes = sizes.at[1:1 + 2 * couples:2].set(source_of - moved).at[2:2 + 2 * couples:2].set(taker + moved)
    return sizes[jax.random.permutation(jax.random.fold_in(stream_key, 2), amount)]


def bell_draw(key, shape, deviation, limit, cuts=(), kind=jnp.bfloat16):
    values = deviation * jax.random.normal(key, shape, jnp.float32)
    if cuts:
        values = values * level_of(key, shape, cuts, -0.22, 0.18)
    return jnp.clip(values, -limit, limit).astype(kind)


def setup_inputs(seed: int = 0) -> dict:
    keys = jax.random.split(jax.random.key(seed), 7)
    query = draw_query(jax.random.fold_in(keys[6], 71), 0)
    key_cache = draw_key_cache(jax.random.fold_in(keys[6], 71), 0)
    value_cache = bell_draw(keys[2], (CACHE, KVH, HD), 1.0, 6.0, ((0, 64), (1, 4)))
    lengths = ragged_sizes(keys[3], N_SEQ, N_SEQ * CACHE_DEV * 3 // 4, CACHE_DEV, 2).astype(jnp.int32)
    out_weight = draw_out_weight(jax.random.fold_in(keys[6], 71), 0)
    norm_gain = jnp.clip(1.0 + 0.18 * jax.random.normal(keys[5], (D,), jnp.float32), 0.1, 1.9)
    return dict(query=query, key_cache=key_cache, value_cache=value_cache, lengths=lengths, out_weight=out_weight, norm_gain=norm_gain)


def reference(query, key_cache, value_cache, lengths, out_weight, norm_gain):
    block_count = CACHE // CACHE_DEV
    group_size = HEADS // KVH
    score_scale = float(QPRE) ** (-0.5)
    grouped = query.astype(jnp.float32).reshape(QTOK, KVH, group_size, HD)
    key_blocks = key_cache.reshape(block_count, CACHE_DEV, KVH, HD)
    value_blocks = value_cache.reshape(block_count, CACHE_DEV, KVH, HD)

    def one_block(running, pieces):
        peak_run, total_run, acc_run = running
        key_block, value_block, length_here = pieces
        scores = jnp.einsum('tkgd,ckd->kgtc', grouped, key_block.astype(jnp.float32)) * score_scale
        inside = jnp.arange(CACHE_DEV, dtype=jnp.int32) < length_here
        scores = jnp.where(inside, scores, jnp.float32(-1e+30))
        block_max = lax.optimization_barrier(jnp.max(scores, axis=-1))
        weights = jnp.where(inside, jnp.exp(scores - block_max[..., None]), jnp.float32(0.0))
        block_sum = lax.optimization_barrier(jnp.sum(weights, axis=-1))
        weights_low = lax.optimization_barrier(weights.astype(jnp.bfloat16))
        block_acc = jnp.einsum('kgtc,ckd->kgtd', weights_low.astype(jnp.float32), value_block.astype(jnp.float32))
        new_peak = jnp.maximum(peak_run, block_max)
        old_factor = jnp.exp(peak_run - new_peak)
        new_factor = jnp.exp(block_max - new_peak)
        total_new = old_factor * total_run + new_factor * block_sum
        acc_new = old_factor[..., None] * acc_run + new_factor[..., None] * block_acc
        return ((new_peak, total_new, acc_new), None)
    start_state = (jnp.full((KVH, group_size, QTOK), -1e+30, jnp.float32), jnp.zeros((KVH, group_size, QTOK), jnp.float32), jnp.zeros((KVH, group_size, QTOK, HD), jnp.float32))
    final_state, unused = lax.scan(one_block, start_state, (key_blocks, value_blocks, lengths.astype(jnp.int32)))
    peak_all, total_all, combined = final_state
    attention = combined / total_all[..., None]
    attention = jnp.transpose(attention, (2, 0, 1, 3)).reshape(QTOK, HEADS * HD).astype(jnp.bfloat16)
    projected = jnp.dot(attention, out_weight.T, preferred_element_type=jnp.float32)
    mean_square = lax.optimization_barrier(jnp.mean(projected * projected, axis=-1))
    normed = projected * lax.rsqrt(mean_square + 1e-06)[:, None] * norm_gain.astype(jnp.float32)[None, :]
    return normed.astype(jnp.bfloat16)
```

```python
import functools

import jax
import jax.numpy as jnp
from jax import lax
from jax.experimental import pallas as pl
from jax.experimental.pallas import tpu as pltpu
from jax.sharding import PartitionSpec as P

D = 4608
QPRE = 144
NZ = 8
NJ = 8
NX = 4
HD = 128
TOK = 128
ROWS = 72
DZ = HD // NZ
MESH = pl.DeviceIdType.MESH


def kernel(
    acc_ref,
    stat_ref,
    weight_ref,
    out_ref,
    got1,
    gstat1,
    weights,
    send2,
    sstat2,
    got2,
    gstat2,
    attn,
    send4,
    got4,
    got5,
    got6,
    got7,
    s1,
    r1,
    t1,
    q1,
    sw,
    rw,
    s2,
    r2,
    t2,
    q2,
    s3,
    r3,
    s4,
    r4,
    s5,
    r5,
    s6,
    r6,
    s7,
    r7,
):
    seq = lax.axis_index("seq")
    x = lax.axis_index("head")
    j = lax.rem(seq, NJ)
    z = lax.div(seq, NJ)

    def peer_j(k):
        return lax.rem(j + k, NJ)

    def peer_z(k):
        return lax.rem(z + k, NZ)

    def peer_x(k):
        return lax.rem(x + k, NX)

    def at_j(p):
        return (z * NJ + p, x)

    def at_z(p):
        return (p * NJ + j, x)

    def at_x(p):
        return (seq, p)

    barrier = pltpu.get_barrier_semaphore()
    for k in range(1, NJ):
        pl.semaphore_signal(barrier, inc=1, device_id=at_j(peer_j(k)), device_id_type=MESH)
    for k in range(1, NZ):
        pl.semaphore_signal(barrier, inc=1, device_id=at_z(peer_z(k)), device_id_type=MESH)
    for k in range(1, NX):
        pl.semaphore_signal(barrier, inc=1, device_id=at_x(peer_x(k)), device_id_type=MESH)
    pl.semaphore_wait(barrier, NJ + NZ + NX - 3)

    def copy(src, dst, ssem, rsem, device):
        return pltpu.make_async_remote_copy(
            src_ref=src, dst_ref=dst, send_sem=ssem, recv_sem=rsem, device_id=device, device_id_type=MESH
        )

    far_j = (4, 3, 5, 2, 6, 1, 7)
    far_z = (4, 3, 5, 2, 6, 1, 7)
    sends = []

    def exchange(src, dst, ssem, rsem, mine, order, peer, place):
        for k in order:
            p = peer(k)
            c = copy(src(p), dst.at[mine], ssem.at[k], rsem.at[mine], place(p))
            c.start()
            sends.append(c)

    def arrived(src, dst, ssem, rsem, order, peer, place):
        for k in order:
            p = peer(k)
            copy(src, dst.at[p], ssem.at[k], rsem.at[p], place(p)).wait_recv()

    exchange(lambda p: stat_ref.at[p], gstat1, t1, q1, j, far_j, peer_j, at_j)
    exchange(lambda p: acc_ref.at[p], got1, s1, r1, j, far_j, peer_j, at_j)
    exchange(
        lambda p: weight_ref.at[:, pl.ds(pl.multiple_of(p * HD, HD), HD)], weights, sw, rw, j, far_j, peer_j, at_j
    )
    gstat1[j] = stat_ref[j]
    got1[j] = acc_ref[j]
    weights[j] = weight_ref[:, pl.ds(pl.multiple_of(j * HD, HD), HD)]
    arrived(stat_ref.at[0], gstat1, t1, q1, far_j[::-1], peer_j, at_j)
    arrived(acc_ref.at[0], got1, s1, r1, far_j[::-1], peer_j, at_j)

    def merged(got, gstat, count):
        tops = [gstat[p, 0:1, :] for p in range(count)]
        top = functools.reduce(jnp.maximum, tops)
        total, value = None, None
        for p in range(count):
            factor = jnp.exp(tops[p] - top)
            one = factor * gstat[p, 1:2, :]
            many = factor * got[p].astype(jnp.float32)
            total = one if total is None else total + one
            value = many if value is None else value + many
        return top, total, value

    top, total, value = merged(got1, gstat1, NJ)
    sstat2[0:1, :] = top
    sstat2[1:2, :] = total
    for p in range(NZ):
        send2[p] = value[p * DZ : (p + 1) * DZ, :].astype(jnp.bfloat16)

    exchange(lambda p: sstat2, gstat2, t2, q2, z, far_z, peer_z, at_z)
    exchange(lambda p: send2.at[p], got2, s2, r2, z, far_z, peer_z, at_z)
    gstat2[z] = sstat2[...]
    got2[z] = send2[z]
    arrived(sstat2, gstat2, t2, q2, far_z[::-1], peer_z, at_z)
    arrived(send2.at[0], got2, s2, r2, far_z[::-1], peer_z, at_z)
    top, total, value = merged(got2, gstat2, NZ)
    attn[z] = (value / total).astype(jnp.bfloat16)

    exchange(lambda p: attn.at[z], attn, s3, r3, z, far_z, peer_z, at_z)
    arrived(weight_ref.at[:, pl.ds(0, HD)], weights, sw, rw, far_j[::-1], peer_j, at_j)
    arrived(attn.at[0], attn, s3, r3, far_z[::-1], peer_z, at_z)

    whole = jnp.concatenate([attn[p] for p in range(NZ)], axis=0)
    for p in range(NJ):
        send4[p] = jnp.dot(weights[p], whole, preferred_element_type=jnp.float32).astype(jnp.bfloat16)
    exchange(lambda p: send4.at[p], got4, s4, r4, j, far_j, peer_j, at_j)
    got4[j] = send4[j]
    arrived(send4.at[0], got4, s4, r4, far_j[::-1], peer_j, at_j)
    part = functools.reduce(jnp.add, [got4[p].astype(jnp.float32) for p in range(NJ)])

    got5[x] = part.astype(jnp.bfloat16)
    exchange(lambda p: got5.at[x], got5, s5, r5, x, (2, 1, 3), peer_x, at_x)
    arrived(got5.at[0], got5, s5, r5, (1, 3, 2), peer_x, at_x)
    projected = functools.reduce(jnp.add, [got5[p].astype(jnp.float32) for p in range(NX)])

    got6[j] = jnp.sum(projected * projected, axis=0, keepdims=True)
    exchange(lambda p: got6.at[j], got6, s6, r6, j, far_j, peer_j, at_j)
    arrived(got6.at[0], got6, s6, r6, far_j[::-1], peer_j, at_j)
    got7[z] = functools.reduce(jnp.add, [got6[p] for p in range(NJ)])
    exchange(lambda p: got7.at[z], got7, s7, r7, z, far_z, peer_z, at_z)
    arrived(got7.at[0], got7, s7, r7, far_z[::-1], peer_z, at_z)
    square = functools.reduce(jnp.add, [got7[p] for p in range(NZ)])
    out_ref[...] = projected * lax.rsqrt(square * (1.0 / D) + 1e-06)

    for c in sends:
        c.wait_send()


def communicate(acc, stat, weight):
    bf16, f32 = jnp.bfloat16, jnp.float32
    dma = pltpu.SemaphoreType.DMA
    j2, z2, x2 = [dma((NJ,))] * 2, [dma((NZ,))] * 2, [dma((NX,))] * 2
    vmem = pl.BlockSpec(memory_space=pltpu.VMEM)
    return pl.pallas_call(
        kernel,
        out_shape=jax.ShapeDtypeStruct((ROWS, TOK), f32),
        in_specs=[vmem] * 3,
        out_specs=vmem,
        scratch_shapes=[
            pltpu.VMEM((NJ, HD, TOK), bf16),
            pltpu.VMEM((NJ, 2, TOK), f32),
            pltpu.VMEM((NJ, ROWS, HD), bf16),
            pltpu.VMEM((NZ, DZ, TOK), bf16),
            pltpu.VMEM((2, TOK), f32),
            pltpu.VMEM((NZ, DZ, TOK), bf16),
            pltpu.VMEM((NZ, 2, TOK), f32),
            pltpu.VMEM((NZ, DZ, TOK), bf16),
            pltpu.VMEM((NJ, ROWS, TOK), bf16),
            pltpu.VMEM((NJ, ROWS, TOK), bf16),
            pltpu.VMEM((NX, ROWS, TOK), bf16),
            pltpu.VMEM((NJ, 1, TOK), f32),
            pltpu.VMEM((NZ, 1, TOK), f32),
            *j2, *j2, *j2, *z2, *z2, *z2, *j2, *x2, *j2, *z2,
        ],
        compiler_params=pltpu.CompilerParams(collective_id=0, has_side_effects=True),
    )(acc, stat, weight)


def body(query, key_cache, value_cache, lengths, out_weight, norm_gain):
    tok_count, heads_local, head_dim = query.shape
    key_count, kv_local, unused_dim = key_cache.shape
    group_size = heads_local // kv_local
    score_scale = float(QPRE) ** (-0.5)
    grouped = query.reshape(tok_count, kv_local, group_size, head_dim)
    scores = (
        jnp.einsum("tkgd,ckd->kgtc", grouped, key_cache, preferred_element_type=jnp.float32)
        * score_scale
    )
    inside = lax.iota(jnp.int32, key_count) < lengths[0]
    scores = jnp.where(inside, scores, jnp.float32(-1e30))
    block_max = jnp.max(scores, axis=-1)
    weights = jnp.where(inside, jnp.exp(scores - block_max[..., None]), jnp.float32(0.0))
    block_sum = jnp.sum(weights, axis=-1)
    weighted = jnp.einsum(
        "kgtc,ckd->kgdt", weights.astype(jnp.bfloat16), value_cache, preferred_element_type=jnp.float32
    )
    acc = weighted.astype(jnp.bfloat16).reshape(heads_local, head_dim, tok_count)
    stat = jnp.stack([block_max, block_sum], axis=2).reshape(heads_local, 2, tok_count)
    normed = communicate(acc, stat, out_weight)
    return (normed * norm_gain[:, None]).astype(jnp.bfloat16).T


def solution(mesh):
    placed = (
        P(None, "head", None),
        P("seq", "head", None),
        P("seq", "head", None),
        P("seq"),
        P("seq", "head"),
        P("seq"),
    )
    return jax.shard_map(
        body, mesh=mesh, in_specs=placed, out_specs=P(None, "seq"), check_vma=False
    )
```

```python
import functools

import jax
import jax.numpy as jnp
from jax import lax
from jax.experimental import pallas as pl
from jax.experimental.pallas import tpu as pltpu
from jax.sharding import PartitionSpec as P

D = 4608
QPRE = 144
NZ = 8
NJ = 8
NX = 4
NS = 64
HD = 128
TOK = 128
ROWS = 72
DZ = HD // NZ
KV = 4
KEYS = 2048
PARTS = 4
STEP = QPRE ** -0.5 * 1.4426950408889634
MESH = pl.DeviceIdType.MESH


def kernel(
    length_ref,
    query_ref,
    key_ref,
    value_ref,
    weight_ref,
    out_ref,
    key_low,
    value_low,
    keys,
    values,
    queries,
    acc_ref,
    stat_ref,
    got1,
    gstat1,
    weights,
    send2,
    sstat2,
    got2,
    gstat2,
    attn,
    send4,
    got4,
    got5,
    got6,
    ck,
    cv,
    cw,
    s1,
    r1,
    t1,
    q1,
    sw,
    rw,
    s2,
    r2,
    t2,
    q2,
    s3,
    r3,
    s4,
    r4,
    s5,
    r5,
    s6,
    r6,
):
    seq = lax.axis_index("seq")
    x = lax.axis_index("head")
    j = lax.rem(seq, NJ)
    z = lax.div(seq, NJ)
    y = lax.div(j, 2)

    part = KEYS * KV // PARTS
    key_copies = [
        pltpu.make_async_copy(key_ref.at[pl.ds(i * part, part)], key_low.at[pl.ds(i * part, part)], ck.at[i])
        for i in range(PARTS)
    ]
    value_copies = [
        pltpu.make_async_copy(value_ref.at[pl.ds(i * part, part)], value_low.at[pl.ds(i * part, part)], cv.at[i])
        for i in range(PARTS)
    ]
    for c in key_copies + value_copies:
        c.start()

    def peer_j(k):
        return lax.rem(j + k, NJ)

    def peer_z(k):
        return lax.rem(z + k, NZ)

    def peer_s(k):
        return lax.rem(seq + k, NS)

    def peer_x(k):
        return lax.rem(x + k, NX)

    def at_j(p):
        return (z * NJ + p, x)

    def at_z(p):
        return (p * NJ + j, x)

    def at_s(p):
        return (p, x)

    def at_x(p):
        return (seq, p)

    barrier = pltpu.get_barrier_semaphore()
    for k in range(1, NS):
        pl.semaphore_signal(barrier, inc=1, device_id=at_s(peer_s(k)), device_id_type=MESH)
    for k in range(1, NX):
        pl.semaphore_signal(barrier, inc=1, device_id=at_x(peer_x(k)), device_id_type=MESH)

    def copy(src, dst, ssem, rsem, device):
        return pltpu.make_async_remote_copy(
            src_ref=src, dst_ref=dst, send_sem=ssem, recv_sem=rsem, device_id=device, device_id_type=MESH
        )

    far_j = (4, 3, 5, 2, 6, 1, 7)
    far_z = (4, 3, 5, 2, 6, 1, 7)
    sends = []

    def exchange(src, dst, ssem, rsem, mine, order, peer, place):
        for k in order:
            p = peer(k)
            c = copy(src(p), dst.at[mine], ssem.at[k], rsem.at[mine], place(p))
            c.start()
            sends.append(c)

    def arrived(src, dst, ssem, rsem, order, peer, place):
        for k in order:
            p = peer(k)
            copy(src, dst.at[p], ssem.at[k], rsem.at[p], place(p)).wait_recv()

    queries[...] = query_ref[...].astype(jnp.float32)
    for i in range(PARTS):
        key_copies[i].wait()
        keys[i * part : (i + 1) * part, :] = key_low[i * part : (i + 1) * part, :].astype(jnp.float32)
    for i in range(PARTS):
        value_copies[i].wait()
        values[i * part : (i + 1) * part, :] = value_low[i * part : (i + 1) * part, :].astype(jnp.float32)

    pl.semaphore_wait(barrier, NS + NX - 2)
    exchange(
        lambda p: weight_ref.at[:, pl.ds(pl.multiple_of(p * HD, HD), HD)], weights, sw, rw, j, far_j, peer_j, at_j
    )
    own_weight = pltpu.make_async_copy(
        weight_ref.at[:, pl.ds(pl.multiple_of(j * HD, HD), HD)], weights.at[j], cw
    )
    own_weight.start()
    length = length_ref[0]

    def attend(h):
        key = keys[pl.ds(h, KEYS, stride=KV), :].astype(jnp.bfloat16)
        query = jnp.concatenate(
            [queries[pl.ds(2 * h + g, TOK, stride=NJ), :].astype(jnp.bfloat16) for g in range(2)], axis=0
        )
        scores = lax.dot_general(key, query, (((1,), (1,)), ((), ())), preferred_element_type=jnp.float32)
        place = lax.broadcasted_iota(jnp.int32, (KEYS, 2 * TOK), 0)
        scores = jnp.where(place < length, scores, -1e30)
        top = jnp.max(scores, axis=0, keepdims=True)
        soft = jnp.exp2((scores - top) * STEP)
        total = jnp.sum(soft, axis=0, keepdims=True)
        value = values[pl.ds(h, KEYS, stride=KV), :].astype(jnp.bfloat16)
        acc = lax.dot_general(
            value, soft.astype(jnp.bfloat16), (((0,), (0,)), ((), ())), preferred_element_type=jnp.float32
        )
        for g in range(2):
            side = slice(g * TOK, (g + 1) * TOK)
            acc_ref[2 * h + g] = acc[:, side].astype(jnp.bfloat16)
            stat_ref[2 * h + g, 0:1, :] = top[:, side] * STEP
            stat_ref[2 * h + g, 1:2, :] = total[:, side]

    def give(p):
        copy(stat_ref.at[p], gstat1.at[j], t1.at[p], q1.at[j], at_j(p)).start()
        copy(acc_ref.at[p], got1.at[j], s1.at[p], r1.at[j], at_j(p)).start()

    def remote(i, carry):
        h = lax.rem(y + 1 + i, KV)
        attend(h)
        give(2 * h)
        give(2 * h + 1)
        return carry

    lax.fori_loop(0, KV - 1, remote, 0)
    attend(y)
    give(4 * y + 1 - j)
    gstat1[j] = stat_ref[j]
    got1[j] = acc_ref[j]
    arrived(stat_ref.at[0], gstat1, t1, q1, far_j[::-1], peer_j, at_j)
    arrived(acc_ref.at[0], got1, s1, r1, far_j[::-1], peer_j, at_j)

    def merged(got, gstat, count):
        tops = [gstat[p, 0:1, :] for p in range(count)]
        top = functools.reduce(jnp.maximum, tops)
        total, value = None, None
        for p in range(count):
            factor = jnp.exp2(tops[p] - top)
            one = factor * gstat[p, 1:2, :]
            many = factor * got[p].astype(jnp.float32)
            total = one if total is None else total + one
            value = many if value is None else value + many
        return top, total, value

    top, total, value = merged(got1, gstat1, NJ)
    sstat2[0:1, :] = top
    sstat2[1:2, :] = total
    for p in range(NZ):
        send2[p] = value[p * DZ : (p + 1) * DZ, :].astype(jnp.bfloat16)

    exchange(lambda p: sstat2, gstat2, t2, q2, z, far_z, peer_z, at_z)
    exchange(lambda p: send2.at[p], got2, s2, r2, z, far_z, peer_z, at_z)
    gstat2[z] = sstat2[...]
    got2[z] = send2[z]
    arrived(sstat2, gstat2, t2, q2, far_z[::-1], peer_z, at_z)
    arrived(send2.at[0], got2, s2, r2, far_z[::-1], peer_z, at_z)
    top, total, value = merged(got2, gstat2, NZ)
    attn[z] = (value / total).astype(jnp.bfloat16)

    exchange(lambda p: attn.at[z], attn, s3, r3, z, far_z, peer_z, at_z)
    own_weight.wait()
    arrived(weight_ref.at[:, pl.ds(0, HD)], weights, sw, rw, far_j[::-1], peer_j, at_j)
    arrived(attn.at[0], attn, s3, r3, far_z[::-1], peer_z, at_z)

    whole = jnp.concatenate([attn[p] for p in range(NZ)], axis=0)
    for p in range(NJ):
        send4[p] = jnp.dot(weights[p], whole, preferred_element_type=jnp.float32).astype(jnp.bfloat16)
    exchange(lambda p: send4.at[p], got4, s4, r4, j, far_j, peer_j, at_j)
    got4[j] = send4[j]
    arrived(send4.at[0], got4, s4, r4, far_j[::-1], peer_j, at_j)
    part = functools.reduce(jnp.add, [got4[p].astype(jnp.float32) for p in range(NJ)])

    got5[x] = part.astype(jnp.bfloat16)
    exchange(lambda p: got5.at[x], got5, s5, r5, x, (2, 1, 3), peer_x, at_x)
    arrived(got5.at[0], got5, s5, r5, (1, 3, 2), peer_x, at_x)
    projected = functools.reduce(jnp.add, [got5[p].astype(jnp.float32) for p in range(NX)])

    got6[seq] = jnp.sum(projected * projected, axis=0, keepdims=True)
    exchange(lambda p: got6.at[seq], got6, s6, r6, seq, range(1, NS), peer_s, at_s)
    arrived(got6.at[0], got6, s6, r6, range(1, NS), peer_s, at_s)
    square = functools.reduce(jnp.add, [got6[p] for p in range(NS)])
    out_ref[...] = projected * lax.rsqrt(square * (1.0 / D) + 1e-06)

    for c in sends:
        c.wait_send()
    for k in range(1, NJ):
        p = peer_j(k)
        copy(stat_ref.at[p], gstat1.at[j], t1.at[p], q1.at[j], at_j(p)).wait_send()
        copy(acc_ref.at[p], got1.at[j], s1.at[p], r1.at[j], at_j(p)).wait_send()


def fused(length, query, key, value, weight):
    bf16, f32 = jnp.bfloat16, jnp.float32
    dma = pltpu.SemaphoreType.DMA
    j2, z2, x2, a2 = [dma((NJ,))] * 2, [dma((NZ,))] * 2, [dma((NX,))] * 2, [dma((NS,))] * 2
    vmem = pl.BlockSpec(memory_space=pltpu.VMEM)
    hbm = pl.BlockSpec(memory_space=pl.ANY)
    return pl.pallas_call(
        kernel,
        out_shape=jax.ShapeDtypeStruct((ROWS, TOK), f32),
        in_specs=[pl.BlockSpec(memory_space=pltpu.SMEM), vmem, hbm, hbm, hbm],
        out_specs=vmem,
        scratch_shapes=[
            pltpu.VMEM((KEYS * KV, HD), bf16),
            pltpu.VMEM((KEYS * KV, HD), bf16),
            pltpu.VMEM((KEYS * KV, HD), f32),
            pltpu.VMEM((KEYS * KV, HD), f32),
            pltpu.VMEM((TOK * NJ, HD), f32),
            pltpu.VMEM((NJ, HD, TOK), bf16),
            pltpu.VMEM((NJ, 2, TOK), f32),
            pltpu.VMEM((NJ, HD, TOK), bf16),
            pltpu.VMEM((NJ, 2, TOK), f32),
            pltpu.VMEM((NJ, ROWS, HD), bf16),
            pltpu.VMEM((NZ, DZ, TOK), bf16),
            pltpu.VMEM((2, TOK), f32),
            pltpu.VMEM((NZ, DZ, TOK), bf16),
            pltpu.VMEM((NZ, 2, TOK), f32),
            pltpu.VMEM((NZ, DZ, TOK), bf16),
            pltpu.VMEM((NJ, ROWS, TOK), bf16),
            pltpu.VMEM((NJ, ROWS, TOK), bf16),
            pltpu.VMEM((NX, ROWS, TOK), bf16),
            pltpu.VMEM((NS, 1, TOK), f32),
            dma((PARTS,)),
            dma((PARTS,)),
            dma(()),
            *j2, *j2, *j2, *z2, *z2, *z2, *j2, *x2, *a2,
        ],
        compiler_params=pltpu.CompilerParams(
            collective_id=0, has_side_effects=True, vmem_limit_bytes=60 * 2**20
        ),
    )(length, query, key, value, weight)


def body(query, key_cache, value_cache, lengths, out_weight, norm_gain):
    normed = fused(
        lengths,
        query.reshape(TOK * NJ, HD),
        key_cache.reshape(KEYS * KV, HD),
        value_cache.reshape(KEYS * KV, HD),
        out_weight,
    )
    return (normed * norm_gain[:, None]).astype(jnp.bfloat16).T


def solution(mesh):
    placed = (
        P(None, "head", None),
        P("seq", "head", None),
        P("seq", "head", None),
        P("seq"),
        P("seq", "head"),
        P("seq"),
    )
    return jax.shard_map(
        body, mesh=mesh, in_specs=placed, out_specs=P(None, "seq"), check_vma=False
    )
```
